32 devices in a mesh: members: 2 (over y), elem: 4 (over z), lev: 4 (over x, core).
Axes of the slice: x: 2, y: 2, z: 4, core: 2. Of those that a mesh axis runs over, the one named last changes fastest.
Arguments:
- tracers: float32 [25, 8, 16, 2048], P(None, 'lev', None, ('members', 'elem')), parts along dimension 3, may hold values from -6 to 6
- layer_mass: float32 [8, 16, 2048], P('lev', None, ('members', 'elem')), parts along dimension 2, may hold values from 0.3 to 2.7
- winds: float32 [2, 8, 16, 2048], P(None, 'lev', None, ('members', 'elem')), parts along dimension 3, may hold values from 0.5 to 1.5
- metric: float32 [16, 1024], P(None, 'elem'), may hold values from 0.6 to 1.6
- neighbours: int32 [1024, 8], P('elem'), may hold values from 0 to 1023, as said below
Outputs:
- tracers_out: float32 [25, 8, 16, 2048], P(None, 'lev', None, ('members', 'elem')), parts along dimension 3
- surface: float32 [16, 2048], P(None, ('members', 'elem')), parts along dimension 1
The draws below stay inside these ranges and needn't reach their ends.
There are 2 independent parts, one for each index of `members`. The reference program is written for one: setup_inputs(seed, part) draws one part's arguments, and reference() takes and returns one part's arrays. A program takes and returns all parts, laid end to end along the dimension named above; an argument that names none is the same for every part. Nothing has to cross between parts.
Inputs may be any that keep to these rules, and one draw needn't show every extreme that they name: `neighbours`: the grid has 32 columns and 32 rows of elements; it is periodic north to south, and east of column 31 of row y lies column 0 of row y + 16 (rows modulo 32). Block b of 256 elements along elem is the square patch of 16 by 16 elements in patch row b // 2 and patch column b % 2, its elements in a drawn order; so the east, west, north and south patches of block b are blocks b + 1, b - 1, b + 2, b - 2 and the diagonal ones b + 3, b + 1, b - 1, b - 2 - 1 (all modulo the number of blocks). Adjacency is symmetric.
All inputs are finite; a program needn't handle non-finite values.
Results may differ from the reference program's by a relative error of at most 0.0003.
Values sent between devices are 32-bit elements; how exact they have to be, the bound alone decides.
A program may use at most 128 MiB of HBM per device.

```python
import math
import jax
import jax.numpy as jnp
import numpy as np
from jax import lax

NTRC = 25
PSIDE = 16
E_DEV = 256
PGX = 2
GX = 32
GY = 32
NE = 1024
NLEV = 8
N_ELEM = 4


def draw_layer_mass(key, part):
    first = jax.random.fold_in(key, 0)
    level = jnp.arange(NLEV).astype(jnp.float32)[:, None, None]
    profile = 0.5 * (1.0 + 2.0 * level / max(NLEV - 1, 1))
    rough = jax.random.uniform(first, (NLEV, 16, NE), jnp.float32, 0.8, 1.2)
    return profile * rough


def draw_neighbours(key, part):
    keys = jax.random.split(jax.random.fold_in(key, 7), N_ELEM)

    def shuffle(block_key):
        return jax.random.permutation(block_key, E_DEV).astype(jnp.int32)
    orders = jax.vmap(shuffle)(keys)
    rows_grid = jnp.broadcast_to(jnp.arange(GY, dtype=jnp.int32)[:, None], (GY, GX))
    cols_grid = jnp.broadcast_to(jnp.arange(GX, dtype=jnp.int32)[None, :], (GY, GX))

    def identity_of(column, row):
        device = row // PSIDE * PGX + column // PSIDE
        inside = row % PSIDE * PSIDE + column % PSIDE
        return device * E_DEV + orders[device, inside]

    def beside(step_x, step_y):
        column = cols_grid + step_x
        row = rows_grid + step_y
        row = jnp.where(column >= GX, row + PSIDE, row)
        row = jnp.where(column < 0, row - PSIDE, row)
        return identity_of(column % GX, row % GY)
    table = jnp.stack([beside(1, 0), beside(-1, 0), beside(0, 1), beside(0, -1), beside(1, 1), beside(-1, 1), beside(1, -1), beside(-1, -1)], axis=-1)
    own = identity_of(cols_grid, rows_grid)
    result = jnp.zeros((NE, 8), jnp.int32)
    return result.at[own.reshape(-1)].set(table.reshape(-1, 8))


def steps_of(key, dims, shards, least, top_value):
    def one(position, shards_of):
        draws = jax.random.uniform(jax.random.fold_in(jax.random.fold_in(key, 6), position), (shards_of,), jnp.float32, least / len(shards), top_value / len(shards))
        return jnp.repeat(jnp.exp(draws), dims[position] // shards_of).reshape((-1,) + (1,) * (len(dims) - position - 1))

    loudness = one(*shards[0])
    for cut in shards[1:]:
        loudness = loudness * one(*cut)
    return loudness


def bell_draw(own_key, dims, deviation, limit, cuts=(), held_as=jnp.bfloat16):
    drawn = jax.random.normal(own_key, dims, jnp.float32) * deviation
    if len(cuts) > 0:
        drawn = steps_of(own_key, dims, cuts, -0.22, 0.18) * drawn
    return jnp.clip(drawn, min=-limit, max=limit).astype(held_as)


def setup_inputs(seed: int = 0, part: int = 0) -> dict:
    seeds = jax.random.split(jax.random.key(seed), 6)
    part_splits = jax.random.split(jax.random.fold_in(seeds[5], part), 6)
    tracers = bell_draw(part_splits[0], (NTRC, NLEV, 16, NE), 1.0, 6.0, ((1, 4), (3, 4)), jnp.float32)
    layer_mass = draw_layer_mass(jax.random.fold_in(jax.random.fold_in(seeds[5], part), 71), part)
    winds = jnp.clip(0.5 + 1.0 * jax.random.uniform(part_splits[2], (2, NLEV, 16, NE), jnp.float32) ** steps_of(part_splits[2], (2, NLEV, 16, NE), ((1, 4), (3, 4)), -0.2, 0.2), 0.5, 1.5)
    metric = jnp.clip(jnp.exp(math.log(1.6) - 0.98082923 * jax.random.uniform(seeds[3], (16, NE), jnp.float32) ** steps_of(seeds[3], (16, NE), ((1, 4),), -0.2, 0.2)), 0.6, 1.6)
    neighbours = draw_neighbours(jax.random.fold_in(seeds[5], 71), part)
    return {"tracers": tracers, "layer_mass": layer_mass, "winds": winds, "metric": metric, "neighbours": neighbours}


time_step = 0.035

def lagrange_scale(points, which):
    product = 1.0
    for other in range(4):
        if other != which:
            product = product * (points[which] - points[other])
    return product

def node_tables():
    points = np.array([-1.0, -1.0 / math.sqrt(5.0), 1.0 / math.sqrt(5.0), 1.0])
    weights = np.array([1.0, 5.0, 5.0, 1.0]) / 6.0
    derivative = np.zeros((4, 4))
    for target in range(4):
        for source in range(4):
            if target == source:
                derivative[target, source] = sum((1.0 / (points[target] - points[other]) for other in range(4) if other != target))
            else:
                derivative[target, source] = lagrange_scale(points, target) / (lagrange_scale(points, source) * (points[target] - points[source]))
    return (np.kron(np.eye(4), derivative), np.kron(derivative, np.eye(4)), np.kron(weights, weights))

def side_links():
    column = list(range(4))
    return [([4 * step + 3 for step in column], [4 * step for step in column]), ([4 * step for step in column], [4 * step + 3 for step in column]), ([12 + step for step in column], [step for step in column]), ([step for step in column], [12 + step for step in column]), ([15], [0]), ([12], [3]), ([3], [12]), ([0], [15])]

def apply_table(table, field):
    return jnp.einsum('nm,...me->...ne', jnp.asarray(table, jnp.float32), field, precision=lax.Precision.HIGHEST)

def tendency(state, winds, metric):
    along_east, along_north, weights = node_tables()
    east_flux = metric * winds[0] * state
    north_flux = metric * winds[1] * state
    return -(apply_table(along_east, east_flux) + apply_table(along_north, north_flux)) / metric

def assemble(weighted, extended, positions):
    total = weighted
    for direction, pair in enumerate(side_links()):
        picked = jnp.take(extended[:, pair[1], :], positions[:, direction], axis=2)
        total = total.at[:, pair[0], :].add(picked)
    return total

def assembled_rate(state, winds, metric, mass, shared, neighbours):
    rate = tendency(state, winds, metric)
    flat = (mass * rate).reshape((-1,) + rate.shape[2:])
    return (assemble(flat, flat, neighbours) / shared).reshape(rate.shape)

def reference(tracers, layer_mass, winds, metric, neighbours):
    weights = node_tables()[2]
    mass = jnp.asarray(weights, jnp.float32)[:, None] * metric
    shared = assemble(mass[None], mass[None], neighbours)[0]
    start_state = jnp.concatenate([layer_mass[None], tracers * layer_mass[None]], axis=0)
    middle_state = start_state + time_step * assembled_rate(start_state, winds, metric, mass, shared, neighbours)
    final_state = 0.5 * (start_state + middle_state + time_step * assembled_rate(middle_state, winds, metric, mass, shared, neighbours))
    thick = final_state[0]
    carried = final_state[1:]
    levels = thick.shape[0]
    surface = lax.optimization_barrier(jnp.sum(thick, axis=0))
    edges = jnp.arange(levels + 1).astype(jnp.float32)
    fraction = (edges + edges * (edges - 1.0) / (levels - 1)) / (2.0 * levels)
    layers = edges[:-1]
    share = (1.0 + 2.0 * layers / (levels - 1)) / (2.0 * levels)
    above_mass = jnp.concatenate([jnp.zeros_like(surface)[None], jnp.cumsum(thick, axis=0)], axis=0)
    delta = above_mass - surface * fraction[:, None, None]
    ratio = carried / thick
    padded = jnp.pad(ratio, ((0, 0), (1, 1), (0, 0), (0, 0)))
    flux = delta * jnp.where(delta > 0.0, padded[:, :-1], padded[:, 1:])
    result = (carried + flux[:, :-1] - flux[:, 1:]) / (surface * share[:, None, None])
    return (result, surface)
```

```python
import functools
import math

import jax
import jax.numpy as jnp
import numpy as np
from jax import lax
from jax.experimental import pallas as pl
from jax.experimental.pallas import tpu as pltpu
from jax.sharding import PartitionSpec as P

PSIDE = 16
STEP = 0.035
MESH = pl.DeviceIdType.MESH
F32 = jnp.float32
BF16 = jnp.bfloat16

SOURCE = [[0, 4, 8, 12], [3, 7, 11, 15], [0, 1, 2, 3], [12, 13, 14, 15], [0], [3], [12], [15]]
TARGET = [[3, 7, 11, 15], [0, 4, 8, 12], [12, 13, 14, 15], [0, 1, 2, 3], [15], [12], [3], [0]]
OPPOSITE = [1, 0, 3, 2, 7, 6, 5, 4]


def lagrange_scale(points, which):
    product = 1.0
    for other in range(4):
        if other != which:
            product = product * (points[which] - points[other])
    return product


def node_tables():
    points = [-1.0, -1.0 / math.sqrt(5.0), 1.0 / math.sqrt(5.0), 1.0]
    weights = [1.0 / 6.0, 5.0 / 6.0, 5.0 / 6.0, 1.0 / 6.0]
    derivative = np.zeros((4, 4))
    for target in range(4):
        for source in range(4):
            if target == source:
                derivative[target, source] = sum(
                    1.0 / (points[target] - points[other]) for other in range(4) if other != target
                )
            else:
                derivative[target, source] = lagrange_scale(points, target) / (
                    lagrange_scale(points, source) * (points[target] - points[source])
                )
    derivative[np.abs(derivative) < 1e-12] = 0.0
    return derivative, weights


def plan(count):
    across = min(8, max(2, count // 8))
    offsets = [1, -1, across, -across, across + 1, across - 1, 1 - across, -1 - across]
    groups = {}
    for direction, offset in enumerate(offsets):
        groups.setdefault(offset % count, []).append(direction)
    keys = sorted(groups)
    lanes = {}
    for key in keys:
        start = 0
        for direction in groups[key]:
            lanes[direction] = start
            start += 4 * PSIDE if direction < 4 else 1
        assert start <= 128
    return offsets, keys, groups, lanes


def kernel(
    count, nlev, ntrc,
    tr, lm, wind, met, nb, nbt,
    out, surf,
    x0, x1, acc, gat, pck, upk, flag, msg, got, coef, thick, last, column, columns,
    rdn, rup, rlo, rhi, edn, eup, elo, ehi, delta, inv,
    halo_send, halo_recv, col_send, col_recv, up_send, up_recv, dn_send, dn_recv,
):
    width = met.shape[1]
    offsets, keys, groups, lanes = plan(count)
    ngroups = len(keys)
    place = lax.axis_index("elem")
    level = lax.axis_index("lev")
    main = ntrc - 1
    half = 32
    derivative, weights = node_tables()

    rlo[...] = jnp.zeros_like(rlo)
    rhi[...] = jnp.zeros_like(rhi)
    elo[...] = jnp.zeros_like(elo)
    ehi[...] = jnp.zeros_like(ehi)

    barrier = pltpu.get_barrier_semaphore()
    for key in keys:
        pl.semaphore_signal(
            barrier, inc=1, device_id={"elem": lax.rem(place + key, count)}, device_id_type=MESH
        )
    for turn in range(1, nlev):
        pl.semaphore_signal(
            barrier, inc=1, device_id={"lev": lax.rem(level + turn, nlev)}, device_id_type=MESH
        )

    for node in range(16):
        for lev in range(2):
            at = lev * 16 + node
            thin = lm[at : at + 1, :]
            x0[node, lev * half : lev * half + main, :] = (
                tr[0:main, lev, node, :] * thin
            )
            x0[node, lev * half + main : lev * half + half, :] = jnp.zeros(
                (half - main, width), F32
            )
            x0[node, lev * half + main : lev * half + main + 1, :] = (
                tr[main, lev, node : node + 1, :] * thin
            )
            x0[node, lev * half + ntrc : lev * half + ntrc + 1, :] = thin

    sub = lax.broadcasted_iota(jnp.int32, (width, width), 0)
    lane = lax.broadcasted_iota(jnp.int32, (width, width), 1)
    for d in range(8):
        base = lax.rem(place + offsets[d] % count, count) * width
        row = nbt[d : d + 1, :] - base
        frow = (row >= 0) & (row < width)
        flag[d : d + 1, :] = jnp.where(frow, 1.0, 0.0)
        if d >= 4:
            continue
        col = nb[:, d : d + 1] - base
        fcol = (col >= 0) & (col < width)
        own = nbt[d : d + 1, :] - place * width
        gat[d] = jnp.where(sub == own, 1.0, 0.0).astype(BF16)
        placed = jnp.where(fcol, col, 2 * width)
        rank = jnp.sum(jnp.where(placed < row, 1.0, 0.0), axis=0, keepdims=True)
        rank = jnp.where(frow, rank, -1.0)
        slot = (lax.broadcasted_iota(jnp.int32, (128, width), 0) & (PSIDE - 1)).astype(F32)
        upk[d] = jnp.where(slot == rank, 1.0, 0.0).astype(BF16)
        order = jnp.sum(
            jnp.where(lane < sub, jnp.where(frow, 1.0, 0.0), 0.0), axis=1, keepdims=True
        )
        order = jnp.where(fcol, order, -1.0)
        slot = (lax.broadcasted_iota(jnp.int32, (width, 128), 1) & (PSIDE - 1)).astype(F32)
        pck[OPPOSITE[d]] = jnp.where(slot == order, 1.0, 0.0).astype(BF16)

    def spread(planes, table):
        rows = planes[0].shape[0]
        x = planes[0] if len(planes) == 1 else jnp.concatenate(planes, axis=0)
        high = x.astype(BF16)
        low = (x - high.astype(F32)).astype(BF16)
        y = jnp.dot(jnp.concatenate([high, low], axis=0), table, preferred_element_type=F32)
        y = y[: x.shape[0]] + y[x.shape[0] :]
        return [y[rows * i : rows * (i + 1)] for i in range(len(planes))]

    def weighted(state):
        def chunk(r, carry):
            lev = r // 4
            rows = pl.ds(pl.multiple_of(r * 8, 8), 8)
            total = [None] * 16

            def put(n, value):
                total[n] = value if total[n] is None else total[n] + value

            for n in range(16):
                i, j = n % 4, n // 4
                h = state[n, rows, :] * met[n : n + 1, :]
                f = h * wind[pl.ds(lev * 16 + n, 1), :]
                g = h * wind[pl.ds(32 + lev * 16 + n, 1), :]
                for a in range(4):
                    east = -weights[a] * weights[j] * derivative[a, i]
                    if east != 0.0:
                        put(4 * j + a, f * np.float32(east))
                    north = -weights[i] * weights[a] * derivative[a, j]
                    if north != 0.0:
                        put(4 * a + i, g * np.float32(north))
            for n in range(16):
                acc[n, rows, :] = total[n]
            return carry

        lax.fori_loop(0, 8, chunk, 0)

    lanes128 = lax.broadcasted_iota(jnp.int32, (64, 128), 1)

    def assemble(stage):
        for pair in ((0, 1), (2, 3)):
            ys = [spread([acc[n] for n in SOURCE[d]], gat[d]) for d in pair]
            for d, y in zip(pair, ys):
                for n, v in zip(TARGET[d], y):
                    acc[n] = acc[n] + v
        if stage == 0:
            pl.semaphore_wait(barrier, ngroups + nlev - 1)
        copies = []
        for g, key in enumerate(keys):
            total = jnp.zeros((64, 128), F32)
            for d in groups[key]:
                if d < 4:
                    y = spread([acc[n] for n in SOURCE[d]], pck[d])
                    for j in range(4):
                        group = lanes[d] // PSIDE + j
                        total = jnp.where(lanes128 // PSIDE == group, y[j], total)
                else:
                    o = OPPOSITE[d]
                    value = jnp.sum(acc[SOURCE[d][0]] * flag[o : o + 1, :], axis=1, keepdims=True)
                    total = jnp.where(lanes128 == lanes[d], value, total)
            msg[stage, g] = total
            copy = pltpu.make_async_remote_copy(
                src_ref=msg.at[stage, g],
                dst_ref=got.at[stage, g],
                send_sem=halo_send.at[stage, g],
                recv_sem=halo_recv.at[stage, g],
                device_id={"elem": lax.rem(place + count - key, count)},
                device_id_type=MESH,
            )
            copy.start()
            copies.append(copy)
        for g, key in enumerate(keys):
            copies[g].wait()
            arrived = got[stage, g]
            for d in groups[key]:
                if d < 4:
                    first = lanes[d] // PSIDE
                    parts = [
                        jnp.where(lanes128 // PSIDE == first + j, arrived, 0.0) for j in range(4)
                    ]
                    for n, v in zip(TARGET[d], spread(parts, upk[d])):
                        acc[n] = acc[n] + v
                else:
                    n = TARGET[d][0]
                    at = lanes[d]
                    acc[n] = acc[n] + arrived[:, at : at + 1] * flag[d : d + 1, :]

    weighted(x0)
    for n in range(16):
        w = np.float32(weights[n % 4] * weights[n // 4])
        acc[n, ntrc + 1 : ntrc + 2, :] = met[n : n + 1, :] * w
    assemble(0)
    for n in range(16):
        c = STEP / acc[n, ntrc + 1 : ntrc + 2, :]
        coef[n : n + 1, :] = c
        x1[n] = x0[n] + c * acc[n]
    weighted(x1)
    assemble(1)

    for n in range(16):
        final = 0.5 * (x0[n] + x1[n] + coef[n : n + 1, :] * acc[n])
        x1[n] = final
        for lev in range(2):
            last[lev, n : n + 1, :] = final[lev * half + main : lev * half + ntrc]
            thick[lev, n : n + 1, :] = final[lev * half + ntrc : lev * half + ntrc + 1]

    column[...] = thick[0] + thick[1]
    columns[level] = thick[0] + thick[1]
    col_copies = []
    for turn in range(1, nlev):
        copy = pltpu.make_async_remote_copy(
            src_ref=column,
            dst_ref=columns.at[level],
            send_sem=col_send.at[turn - 1],
            recv_sem=col_recv.at[turn - 1],
            device_id={"lev": lax.rem(level + turn, nlev)},
            device_id_type=MESH,
        )
        copy.start()
        col_copies.append(copy)

    def up_copy(q):
        src, dst = (eup, elo) if q == 4 else (rup.at[pl.ds(4 * q, 4)], rlo.at[pl.ds(4 * q, 4)])
        return pltpu.make_async_remote_copy(
            src_ref=src, dst_ref=dst, send_sem=up_send.at[q], recv_sem=up_recv.at[q],
            device_id={"lev": lax.rem(level + 1, nlev)}, device_id_type=MESH,
        )

    def dn_copy(q):
        src, dst = (edn, ehi) if q == 4 else (rdn.at[pl.ds(4 * q, 4)], rhi.at[pl.ds(4 * q, 4)])
        return pltpu.make_async_remote_copy(
            src_ref=src, dst_ref=dst, send_sem=dn_send.at[q], recv_sem=dn_recv.at[q],
            device_id={"lev": lax.rem(level + nlev - 1, nlev)}, device_id_type=MESH,
        )

    def when_up(fn):
        pl.when(level < nlev - 1)(fn)

    def when_dn(fn):
        pl.when(level > 0)(fn)

    inverse = [1.0 / thick[0], 1.0 / thick[1]]
    edn[...] = last[0] * inverse[0]
    eup[...] = last[1] * inverse[1]
    for q in range(5):
        if q < 4:
            for n in range(4 * q, 4 * q + 4):
                rdn[n] = x1[n, 0:main, :] * inverse[0][n : n + 1]
                rup[n] = x1[n, half : half + main, :] * inverse[1][n : n + 1]
        when_up(lambda: up_copy(q).start())
        when_dn(lambda: dn_copy(q).start())

    for copy in col_copies:
        copy.wait()
    below = jnp.zeros((16, width), F32)
    whole = jnp.zeros((16, width), F32)
    for lev in range(nlev):
        part = columns[lev]
        whole = whole + part
        below = below + jnp.where(lev < level, part, 0.0)
    surf[...] = whole
    nl = 2 * nlev
    above = [below, below + thick[0], below + thick[0] + thick[1]]
    for k in range(3):
        edge = (2 * level + k).astype(F32)
        fraction = (edge + edge * (edge - 1.0) * (1.0 / (nl - 1))) * (1.0 / (2.0 * nl))
        delta[k] = above[k] - whole * fraction
        if k < 2:
            share = (1.0 + 2.0 * edge * (1.0 / (nl - 1))) * (1.0 / (2.0 * nl))
            inv[k] = 1.0 / (whole * share)

    def remap(d, r, carried, scale):
        flux = [d[k] * jnp.where(d[k] > 0.0, r[k], r[k + 1]) for k in range(3)]
        return [(carried[k] + flux[k] - flux[k + 1]) * scale[k] for k in range(2)]

    for q in range(5):
        when_up(lambda: up_copy(q).wait_send())
        when_dn(lambda: dn_copy(q).wait_send())
        when_dn(lambda: up_copy(q).wait_recv())
        when_up(lambda: dn_copy(q).wait_recv())
        if q == 4:
            y = remap(
                [delta[k] for k in range(3)],
                [elo[...], edn[...], eup[...], ehi[...]],
                [last[0], last[1]],
                [inv[0], inv[1]],
            )
            out[main, 0] = y[0]
            out[main, 1] = y[1]
            continue
        for n in range(4 * q, 4 * q + 4):
            y = remap(
                [delta[k, n : n + 1, :] for k in range(3)],
                [rlo[n], rdn[n], rup[n], rhi[n]],
                [x1[n, 0:main, :], x1[n, half : half + main, :]],
                [inv[0, n : n + 1, :], inv[1, n : n + 1, :]],
            )
            out[0:main, 0, n, :] = y[0]
            out[0:main, 1, n, :] = y[1]


def solution(mesh):
    count, nlev = mesh.shape["elem"], mesh.shape["lev"]
    ngroups = len(plan(count)[1])

    def per_device(tracers, layer_mass, winds, metric, neighbours):
        ntrc, here, nodes, width = tracers.shape
        assert here == 2 and nodes == 16 and ntrc == 25
        main = ntrc - 1
        vmem = pl.BlockSpec(memory_space=pltpu.VMEM)
        dma = pltpu.SemaphoreType.DMA
        result, surface = pl.pallas_call(
            functools.partial(kernel, count, nlev, ntrc),
            out_shape=(
                jax.ShapeDtypeStruct(tracers.shape, F32),
                jax.ShapeDtypeStruct((nodes, width), F32),
            ),
            in_specs=[vmem] * 6,
            out_specs=(vmem, vmem),
            scratch_shapes=[
                pltpu.VMEM((nodes, 64, width), F32),
                pltpu.VMEM((nodes, 64, width), F32),
                pltpu.VMEM((nodes, 64, width), F32),
                pltpu.VMEM((4, width, width), BF16),
                pltpu.VMEM((4, width, 128), BF16),
                pltpu.VMEM((4, 128, width), BF16),
                pltpu.VMEM((8, width), F32),
                pltpu.VMEM((2, ngroups, 64, 128), F32),
                pltpu.VMEM((2, ngroups, 64, 128), F32),
                pltpu.VMEM((nodes, width), F32),
                pltpu.VMEM((2, nodes, width), F32),
                pltpu.VMEM((2, nodes, width), F32),
                pltpu.VMEM((nodes, width), F32),
                pltpu.VMEM((nlev, nodes, width), F32),
            ]
            + [pltpu.VMEM((nodes, main, width), F32)] * 4
            + [pltpu.VMEM((nodes, width), F32)] * 4
            + [
                pltpu.VMEM((3, nodes, width), F32),
                pltpu.VMEM((2, nodes, width), F32),
                dma((2, ngroups)),
                dma((2, ngroups)),
                dma((nlev - 1,)),
                dma((nlev - 1,)),
                dma((5,)),
                dma((5,)),
                dma((5,)),
                dma((5,)),
            ],
            compiler_params=pltpu.CompilerParams(collective_id=0, has_side_effects=True),
        )(
            tracers,
            layer_mass.reshape(-1, width),
            winds.reshape(-1, width),
            metric,
            neighbours,
            neighbours.T,
        )
        return result, surface

    placed = (
        P(None, "lev", None, ("members", "elem")),
        P("lev", None, ("members", "elem")),
        P(None, "lev", None, ("members", "elem")),
        P(None, "elem"),
        P("elem", None),
    )
    return jax.shard_map(
        per_device,
        mesh=mesh,
        in_specs=placed,
        out_specs=(P(None, "lev", None, ("members", "elem")), P(None, ("members", "elem"))),
        check_vma=False,
    )
```

```python
import functools
import math

import jax
import jax.numpy as jnp
import numpy as np
from jax import lax
from jax.experimental import pallas as pl
from jax.experimental.pallas import tpu as pltpu
from jax.sharding import PartitionSpec as P

PSIDE = 16
STEP = 0.035
MESH = pl.DeviceIdType.MESH
F32 = jnp.float32
BF16 = jnp.bfloat16

SOURCE = [[0, 4, 8, 12], [3, 7, 11, 15], [0, 1, 2, 3], [12, 13, 14, 15], [0], [3], [12], [15]]
TARGET = [[3, 7, 11, 15], [0, 4, 8, 12], [12, 13, 14, 15], [0, 1, 2, 3], [15], [12], [3], [0]]
OPPOSITE = [1, 0, 3, 2, 7, 6, 5, 4]


def lagrange_scale(points, which):
    product = 1.0
    for other in range(4):
        if other != which:
            product = product * (points[which] - points[other])
    return product


def node_tables():
    points = [-1.0, -1.0 / math.sqrt(5.0), 1.0 / math.sqrt(5.0), 1.0]
    weights = [1.0 / 6.0, 5.0 / 6.0, 5.0 / 6.0, 1.0 / 6.0]
    derivative = np.zeros((4, 4))
    for target in range(4):
        for source in range(4):
            if target == source:
                derivative[target, source] = sum(
                    1.0 / (points[target] - points[other]) for other in range(4) if other != target
                )
            else:
                derivative[target, source] = lagrange_scale(points, target) / (
                    lagrange_scale(points, source) * (points[target] - points[source])
                )
    derivative[np.abs(derivative) < 1e-12] = 0.0
    return derivative, weights


def plan(count):
    across = min(8, max(2, count // 8))
    offsets = [1, -1, across, -across, across + 1, across - 1, 1 - across, -1 - across]
    groups = {}
    for direction, offset in enumerate(offsets):
        groups.setdefault(offset % count, []).append(direction)
    keys = sorted(groups)
    lanes = {}
    for key in keys:
        start = 0
        for direction in groups[key]:
            lanes[direction] = start
            start += 4 * PSIDE if direction < 4 else 1
        assert start <= 128
    return offsets, keys, groups, lanes


def kernel(
    count, nlev, ntrc,
    tr_hbm, lm, wind, met, nbt,
    out, surf,
    tr, x0, x1, xn, acc, gat, pck, upk, flag, msg, got, gotn, coef, part, edge, elo, ehi,
    column, columns, delta, inv, thin,
    load_sem, halo_send, halo_recv, far_send, far_recv, col_send, col_recv,
    up_send, up_recv, dn_send, dn_recv,
):
    width = met.shape[1]
    offsets, keys, groups, lanes = plan(count)
    ngroups = len(keys)
    place = lax.axis_index("elem")
    level = lax.axis_index("lev")
    main = ntrc - 1
    half = 32
    derivative, weights = node_tables()

    load = pltpu.make_async_copy(tr_hbm, tr, load_sem)
    load.start()

    xn[...] = jnp.zeros_like(xn)
    gotn[...] = jnp.zeros_like(gotn)
    for ref in (elo, ehi):
        ref[0] = jnp.zeros((16, width), F32)
        ref[1] = jnp.ones((16, width), F32)

    barrier = pltpu.get_barrier_semaphore()
    for key in keys:
        pl.semaphore_signal(
            barrier, inc=1, device_id={"elem": lax.rem(place + key, count)}, device_id_type=MESH
        )
        for turn in (1, nlev - 1):
            pl.semaphore_signal(
                barrier,
                inc=1,
                device_id={
                    "elem": lax.rem(place + key, count),
                    "lev": lax.rem(level + turn, nlev),
                },
                device_id_type=MESH,
            )
    for turn in range(1, nlev):
        pl.semaphore_signal(
            barrier, inc=1, device_id={"lev": lax.rem(level + turn, nlev)}, device_id_type=MESH
        )

    sub = lax.broadcasted_iota(jnp.int32, (width, width), 0)
    lane = lax.broadcasted_iota(jnp.int32, (width, width), 1)
    nb = jnp.transpose(nbt[...].astype(F32)).astype(jnp.int32)
    for d in range(8):
        base = lax.rem(place + offsets[d] % count, count) * width
        row = nbt[d : d + 1, :] - base
        frow = (row >= 0) & (row < width)
        flag[d : d + 1, :] = jnp.where(frow, 1.0, 0.0)
        if d >= 4:
            continue
        col = nb[:, d : d + 1] - base
        fcol = (col >= 0) & (col < width)
        own = nbt[d : d + 1, :] - place * width
        gat[d] = jnp.where(sub == own, 1.0, 0.0).astype(BF16)
        placed = jnp.where(fcol, col, 2 * width)
        rank = jnp.sum(jnp.where(placed < row, 1.0, 0.0), axis=0, keepdims=True)
        rank = jnp.where(frow, rank, -1.0)
        slot = (lax.broadcasted_iota(jnp.int32, (128, width), 0) & (PSIDE - 1)).astype(F32)
        upk[d] = jnp.where(slot == rank, 1.0, 0.0).astype(BF16)
        order = jnp.sum(
            jnp.where(lane < sub, jnp.where(frow, 1.0, 0.0), 0.0), axis=1, keepdims=True
        )
        order = jnp.where(fcol, order, -1.0)
        slot = (lax.broadcasted_iota(jnp.int32, (width, 128), 1) & (PSIDE - 1)).astype(F32)
        pck[OPPOSITE[d]] = jnp.where(slot == order, 1.0, 0.0).astype(BF16)

    load.wait()
    for node in range(16):
        for lev in range(2):
            at = lev * 16 + node
            mass = lm[at : at + 1, :]
            x0[node, lev * half : lev * half + main, :] = (
                tr[0:main, lev, node, :] * mass
            )
            x0[node, lev * half + main : lev * half + half, :] = jnp.zeros(
                (half - main, width), F32
            )
            x0[node, lev * half + main : lev * half + main + 1, :] = (
                tr[main, lev, node : node + 1, :] * mass
            )
            x0[node, lev * half + ntrc : lev * half + ntrc + 1, :] = mass

    def spread(planes, table):
        rows = planes[0].shape[0]
        x = planes[0] if len(planes) == 1 else jnp.concatenate(planes, axis=0)
        high = x.astype(BF16)
        low = (x - high.astype(F32)).astype(BF16)
        y = jnp.dot(jnp.concatenate([high, low], axis=0), table, preferred_element_type=F32)
        y = y[: x.shape[0]] + y[x.shape[0] :]
        return [y[rows * i : rows * (i + 1)] for i in range(len(planes))]

    def weighted(state):
        def chunk(r, carry):
            lev = r // 4
            rows = pl.ds(pl.multiple_of(r * 8, 8), 8)
            total = [None] * 16

            def put(n, value):
                total[n] = value if total[n] is None else total[n] + value

            for n in range(16):
                i, j = n % 4, n // 4
                h = state[n, rows, :] * met[n : n + 1, :]
                f = h * wind[pl.ds(lev * 16 + n, 1), :]
                g = h * wind[pl.ds(32 + lev * 16 + n, 1), :]
                for a in range(4):
                    east = -weights[a] * weights[j] * derivative[a, i]
                    if east != 0.0:
                        put(4 * j + a, f * np.float32(east))
                    north = -weights[i] * weights[a] * derivative[a, j]
                    if north != 0.0:
                        put(4 * a + i, g * np.float32(north))
            for n in range(16):
                acc[n, rows, :] = total[n]
            return carry

        lax.fori_loop(0, 8, chunk, 0)

    lanes128 = lax.broadcasted_iota(jnp.int32, (64, 128), 1)

    def gather():
        for pair in ((0, 1), (2, 3)):
            ys = [spread([acc[n] for n in SOURCE[d]], gat[d]) for d in pair]
            for d, y in zip(pair, ys):
                for n, v in zip(TARGET[d], y):
                    acc[n] = acc[n] + v

    def halo_copy(stage, g):
        return pltpu.make_async_remote_copy(
            src_ref=msg.at[stage, g],
            dst_ref=got.at[stage, g],
            send_sem=halo_send.at[stage, g],
            recv_sem=halo_recv.at[stage, g],
            device_id={"elem": lax.rem(place + count - keys[g], count)},
            device_id_type=MESH,
        )

    def far_copy(g, up):
        return pltpu.make_async_remote_copy(
            src_ref=msg.at[1, g, pl.ds(half * up, half)],
            dst_ref=gotn.at[g, pl.ds(half * (1 - up), half)],
            send_sem=far_send.at[g, up],
            recv_sem=far_recv.at[g, up],
            device_id={
                "elem": lax.rem(place + count - keys[g], count),
                "lev": lax.rem(level + (1 if up else nlev - 1), nlev),
            },
            device_id_type=MESH,
        )

    def when_up(fn):
        pl.when(level < nlev - 1)(fn)

    def when_dn(fn):
        pl.when(level > 0)(fn)

    def send(stage):
        for g, key in enumerate(keys):
            total = jnp.zeros((64, 128), F32)
            for d in groups[key]:
                if d < 4:
                    y = spread([acc[n] for n in SOURCE[d]], pck[d])
                    for j in range(4):
                        group = lanes[d] // PSIDE + j
                        total = jnp.where(lanes128 // PSIDE == group, y[j], total)
                else:
                    o = OPPOSITE[d]
                    value = jnp.sum(acc[SOURCE[d][0]] * flag[o : o + 1, :], axis=1, keepdims=True)
                    total = jnp.where(lanes128 == lanes[d], value, total)
            msg[stage, g] = total
            halo_copy(stage, g).start()

    def receive(arrived, fresh):
        seen = set()
        for g, key in enumerate(keys):
            for d in groups[key]:
                if d < 4:
                    first = lanes[d] // PSIDE
                    parts = [
                        jnp.where(lanes128 // PSIDE == first + j, arrived[g], 0.0)
                        for j in range(4)
                    ]
                    values = spread(parts, upk[d])
                else:
                    at = lanes[d]
                    values = [arrived[g][:, at : at + 1] * flag[d : d + 1, :]]
                for n, v in zip(TARGET[d], values):
                    acc[n] = v if fresh and n not in seen else acc[n] + v
                    seen.add(n)

    weighted(x0)
    for n in range(16):
        w = np.float32(weights[n % 4] * weights[n // 4])
        acc[n, ntrc + 1 : ntrc + 2, :] = met[n : n + 1, :] * w
    gather()
    pl.semaphore_wait(barrier, 3 * ngroups + nlev - 1)
    send(0)
    for g in range(ngroups):
        halo_copy(0, g).wait()
    receive([got[0, g] for g in range(ngroups)], False)
    for n in range(16):
        c = STEP / acc[n, ntrc + 1 : ntrc + 2, :]
        coef[n : n + 1, :] = c
        x1[n] = x0[n] + c * acc[n]
    weighted(x1)
    gather()
    send(1)
    for g in range(ngroups):
        when_up(lambda: far_copy(g, 1).start())
        when_dn(lambda: far_copy(g, 0).start())

    for n in range(16):
        ch = coef[n : n + 1, :] * 0.5
        coef[n : n + 1, :] = ch
        local = 0.5 * (x0[n] + x1[n]) + ch * acc[n]
        x1[n] = local
        for lev in range(2):
            for k in range(2):
                row = lev * half + main + k
                edge[lev, k, n : n + 1, :] = local[row : row + 1]

    def up_copy(q):
        nodes = pl.ds(4 * q, 4)
        src, dst = (
            (edge.at[1], elo)
            if q == 4
            else (x1.at[nodes, pl.ds(half, main)], xn.at[nodes, pl.ds(0, main)])
        )
        return pltpu.make_async_remote_copy(
            src_ref=src, dst_ref=dst, send_sem=up_send.at[q], recv_sem=up_recv.at[q],
            device_id={"lev": lax.rem(level + 1, nlev)}, device_id_type=MESH,
        )

    def dn_copy(q):
        nodes = pl.ds(4 * q, 4)
        src, dst = (
            (edge.at[0], ehi)
            if q == 4
            else (x1.at[nodes, pl.ds(0, main)], xn.at[nodes, pl.ds(half, main)])
        )
        return pltpu.make_async_remote_copy(
            src_ref=src, dst_ref=dst, send_sem=dn_send.at[q], recv_sem=dn_recv.at[q],
            device_id={"lev": lax.rem(level + nlev - 1, nlev)}, device_id_type=MESH,
        )

    for q in (4, 0, 1, 2, 3):
        when_up(lambda: up_copy(q).start())
        when_dn(lambda: dn_copy(q).start())

    for g in range(ngroups):
        halo_copy(1, g).wait()
    receive([got[1, g] for g in range(ngroups)], True)
    inner = (5, 6, 9, 10)
    for n in range(16):
        if n in inner:
            x0[n] = x1[n]
        else:
            x0[n] = x1[n] + coef[n : n + 1, :] * acc[n]
        for lev in range(2):
            for k in range(2):
                row = lev * half + main + k
                part[lev, k, n : n + 1, :] = x0[n, row : row + 1, :]

    thick = [part[0, 1], part[1, 1]]
    column[...] = thick[0] + thick[1]
    columns[level] = thick[0] + thick[1]
    col_copies = []
    for turn in range(1, nlev):
        copy = pltpu.make_async_remote_copy(
            src_ref=column,
            dst_ref=columns.at[level],
            send_sem=col_send.at[turn - 1],
            recv_sem=col_recv.at[turn - 1],
            device_id={"lev": lax.rem(level + turn, nlev)},
            device_id_type=MESH,
        )
        copy.start()
        col_copies.append(copy)

    for g in range(ngroups):
        when_up(lambda: far_copy(g, 1).wait_send())
        when_dn(lambda: far_copy(g, 0).wait_send())
        when_dn(lambda: far_copy(g, 1).wait_recv())
        when_up(lambda: far_copy(g, 0).wait_recv())
    receive([gotn[g] for g in range(ngroups)], True)
    for n in inner:
        acc[n] = jnp.zeros((64, width), F32)

    for copy in col_copies:
        copy.wait()
    below = jnp.zeros((16, width), F32)
    whole = jnp.zeros((16, width), F32)
    for lev in range(nlev):
        piece = columns[lev]
        whole = whole + piece
        below = below + jnp.where(lev < level, piece, 0.0)
    surf[...] = whole
    nl = 2 * nlev
    above = [below, below + thick[0], below + thick[0] + thick[1]]
    for k in range(3):
        place_k = (2 * level + k).astype(F32)
        fraction = (place_k + place_k * (place_k - 1.0) * (1.0 / (nl - 1))) * (1.0 / (2.0 * nl))
        delta[k] = above[k] - whole * fraction
        if k < 2:
            share = (1.0 + 2.0 * place_k * (1.0 / (nl - 1))) * (1.0 / (2.0 * nl))
            inv[k] = 1.0 / (whole * share)

    def remap(d, r, carried, scale):
        flux = [d[k] * jnp.where(d[k] > 0.0, r[k], r[k + 1]) for k in range(3)]
        return [(carried[k] + flux[k] - flux[k + 1]) * scale[k] for k in range(2)]

    for q in (4, 0, 1, 2, 3):
        when_up(lambda: up_copy(q).wait_send())
        when_dn(lambda: dn_copy(q).wait_send())
        when_dn(lambda: up_copy(q).wait_recv())
        when_up(lambda: dn_copy(q).wait_recv())
        if q == 4:
            tail = [[], []]
            for side, ref in enumerate((elo, ehi)):
                for k in range(2):
                    row = side * half + main + k
                    fix = jnp.concatenate([acc[n, row : row + 1, :] for n in range(16)], axis=0)
                    tail[side].append(ref[k] + coef[...] * fix)
            thin[0] = 1.0 / tail[0][1]
            thin[1] = 1.0 / thick[0]
            thin[2] = 1.0 / thick[1]
            thin[3] = 1.0 / tail[1][1]
            carried = [tail[0][0], part[0, 0], part[1, 0], tail[1][0]]
            y = remap(
                [delta[k] for k in range(3)],
                [carried[k] * thin[k] for k in range(4)],
                carried[1:3],
                [inv[0], inv[1]],
            )
            out[main, 0] = y[0]
            out[main, 1] = y[1]
            continue
        for n in range(4 * q, 4 * q + 4):
            ch = coef[n : n + 1, :]
            carried = [
                xn[n, 0:main, :] + ch * acc[n, 0:main, :],
                x0[n, 0:main, :],
                x0[n, half : half + main, :],
                xn[n, half : half + main, :] + ch * acc[n, half : half + main, :],
            ]
            y = remap(
                [delta[k, n : n + 1, :] for k in range(3)],
                [carried[k] * thin[k, n : n + 1, :] for k in range(4)],
                carried[1:3],
                [inv[0, n : n + 1, :], inv[1, n : n + 1, :]],
            )
            out[0:main, 0, n, :] = y[0]
            out[0:main, 1, n, :] = y[1]


def solution(mesh):
    count, nlev = mesh.shape["elem"], mesh.shape["lev"]
    ngroups = len(plan(count)[1])

    def per_device(tracers, layer_mass, winds, metric, neighbours):
        ntrc, here, nodes, width = tracers.shape
        assert here == 2 and nodes == 16 and ntrc == 25
        main = ntrc - 1
        vmem = pl.BlockSpec(memory_space=pltpu.VMEM)
        dma = pltpu.SemaphoreType.DMA
        result, surface = pl.pallas_call(
            functools.partial(kernel, count, nlev, ntrc),
            out_shape=(
                jax.ShapeDtypeStruct(tracers.shape, F32),
                jax.ShapeDtypeStruct((nodes, width), F32),
            ),
            in_specs=[pl.BlockSpec(memory_space=pl.ANY)] + [vmem] * 4,
            out_specs=(vmem, vmem),
            scratch_shapes=[pltpu.VMEM(tracers.shape, F32)]
            + [pltpu.VMEM((nodes, 64, width), F32)] * 4
            + [
                pltpu.VMEM((4, width, width), BF16),
                pltpu.VMEM((4, width, 128), BF16),
                pltpu.VMEM((4, 128, width), BF16),
                pltpu.VMEM((8, width), F32),
                pltpu.VMEM((2, ngroups, 64, 128), F32),
                pltpu.VMEM((2, ngroups, 64, 128), F32),
                pltpu.VMEM((ngroups, 64, 128), F32),
                pltpu.VMEM((nodes, width), F32),
                pltpu.VMEM((2, 2, nodes, width), F32),
                pltpu.VMEM((2, 2, nodes, width), F32),
                pltpu.VMEM((2, nodes, width), F32),
                pltpu.VMEM((2, nodes, width), F32),
                pltpu.VMEM((nodes, width), F32),
                pltpu.VMEM((nlev, nodes, width), F32),
                pltpu.VMEM((3, nodes, width), F32),
                pltpu.VMEM((2, nodes, width), F32),
                pltpu.VMEM((4, nodes, width), F32),
                dma,
                dma((2, ngroups)),
                dma((2, ngroups)),
                dma((ngroups, 2)),
                dma((ngroups, 2)),
                dma((nlev - 1,)),
                dma((nlev - 1,)),
                dma((5,)),
                dma((5,)),
                dma((5,)),
                dma((5,)),
            ],
            compiler_params=pltpu.CompilerParams(collective_id=0, has_side_effects=True),
        )(
            tracers,
            layer_mass.reshape(-1, width),
            winds.reshape(-1, width),
            metric,
            neighbours.T,
        )
        return result, surface

    placed = (
        P(None, "lev", None, ("members", "elem")),
        P("lev", None, ("members", "elem")),
        P(None, "lev", None, ("members", "elem")),
        P(None, "elem"),
        P("elem", None),
    )
    return jax.shard_map(
        per_device,
        mesh=mesh,
        in_specs=placed,
        out_specs=(P(None, "lev", None, ("members", "elem")), P(None, ("members", "elem"))),
        check_vma=False,
    )
```
